8 devices in a mesh: rep: 1 (over z), tp: 2 (over y), dp: 4 (over x, core).
Axes of the slice: x: 2, y: 2, z: 1, core: 2. Of those that a mesh axis runs over, the one named last changes fastest.
Arguments:
- x: bfloat16 [512, 2560], P(('rep', 'dp'))
- lengths: int32 [512], P(('rep', 'dp'))
- cache0: bfloat16 [512, 256, 288], P(('rep', 'dp'))
- cache1: bfloat16 [512, 256, 288], P(('rep', 'dp'))
- attn_gain: float32 [2, 2560], replicated
- kv_gain: float32 [2, 256], replicated
- q_gain: float32 [2, 768], replicated
- ffn_gain: float32 [2, 2560], replicated
- w_dkv: bfloat16 [2, 2560, 288], replicated
- w_qa: bfloat16 [2, 2560, 768], replicated
- w_qb: bfloat16 [2, 768, 3840], P(None, None, 'tp')
- w_uk: bfloat16 [2, 40, 64, 256], P(None, 'tp')
- w_uv: bfloat16 [2, 40, 256, 64], P(None, 'tp')
- w_o: bfloat16 [2, 2560, 2560], P(None, 'tp')
- w_gate: bfloat16 [2, 2560, 6400], replicated
- w_up: bfloat16 [2, 2560, 6400], replicated
- w_down: bfloat16 [2, 6400, 2560], replicated
Outputs:
- output 1: bfloat16 [512, 2560], P(('rep', 'dp'))
- output 2: bfloat16 [512, 256, 288], P(('rep', 'dp'))
- output 3: bfloat16 [512, 256, 288], P(('rep', 'dp'))
All inputs are finite; a program needn't handle non-finite values.
Results may differ from the reference program's by a relative error of at most 0.014556.
Values are sent between devices in bfloat16 or wider.
A program may use at most 1.25 GiB of HBM per device.

```python
import jax
import jax.numpy as jnp
from jax import lax

MODEL_DIM = 2560
FFN_DIM = 6400
NUM_HEADS = 40
Q_LORA = 768
KV_LORA = 256
ROPE_DIM = 32
NOPE_DIM = 64
V_DIM = 64
BATCH = 512
SEQ_LEN = 256
LAYER_COUNT = 2

LAT_WIDTH = KV_LORA + ROPE_DIM
QK_WIDTH = NOPE_DIM + ROPE_DIM
NORM_EPS = 1e-6
ROPE_BASE = 10000.0


def rms_norm(values, gain_vec):
    wide_vals = values.astype(jnp.float32)
    inv_rms = lax.rsqrt(jnp.mean(wide_vals * wide_vals, axis=-1, keepdims=True) + NORM_EPS)
    return (wide_vals * inv_rms * gain_vec.astype(jnp.float32)).astype(jnp.bfloat16)


def rope_tables(lengths):
    half_dim = ROPE_DIM // 2
    inv_freq = ROPE_BASE ** (-2.0 * jnp.arange(half_dim).astype(jnp.float32) / ROPE_DIM)
    angles = lengths.astype(jnp.float32)[:, None] * inv_freq[None, :]
    return jnp.cos(angles), jnp.sin(angles)


def rotate(values, cos_tab, sin_tab):
    half_dim = values.shape[-1] // 2
    first_half = values[..., :half_dim]
    second_half = values[..., half_dim:]
    return jnp.concatenate([first_half * cos_tab - second_half * sin_tab, second_half * cos_tab + first_half * sin_tab], axis=-1)


def row_attention(row_query, row_cache, row_len):
    scores = jnp.einsum('hk,tk->ht', row_query.astype(jnp.float32), row_cache.astype(jnp.float32)) * QK_WIDTH ** -0.5
    valid_mask = jnp.arange(SEQ_LEN)[None, :] <= row_len
    att_probs = jax.nn.softmax(jnp.where(valid_mask, scores, -1e30), axis=-1).astype(jnp.bfloat16)
    return jnp.einsum('ht,tk->hk', att_probs.astype(jnp.float32), row_cache[:, :KV_LORA].astype(jnp.float32)).astype(jnp.bfloat16)


def layer_step(x_rows, lengths, cache, cos_tab, sin_tab, attn_g, kv_g, q_g, ffn_g, w_dkv, w_qa, w_qb, w_uk, w_uv, w_o, w_gate, w_up, w_down):
    normed = rms_norm(x_rows, attn_g)
    kv_lat = jnp.dot(normed, w_dkv, preferred_element_type=jnp.float32)
    new_entry = jnp.concatenate([rms_norm(kv_lat[:, :KV_LORA], kv_g), rotate(kv_lat[:, KV_LORA:], cos_tab, sin_tab).astype(jnp.bfloat16)], axis=-1)
    is_slot = (jnp.arange(SEQ_LEN)[None, :] == lengths[:, None])[:, :, None]
    new_cache = jnp.where(is_slot, new_entry[:, None, :], cache)
    q_low = rms_norm(jnp.dot(normed, w_qa, preferred_element_type=jnp.float32), q_g)
    q_full = jnp.dot(q_low, w_qb, preferred_element_type=jnp.float32).reshape(BATCH, NUM_HEADS, QK_WIDTH)
    q_nope = q_full[:, :, :NOPE_DIM].astype(jnp.bfloat16)
    q_rot = rotate(q_full[:, :, NOPE_DIM:], cos_tab[:, None, :], sin_tab[:, None, :]).astype(jnp.bfloat16)
    q_lat = jnp.einsum('bhn,hnk->bhk', q_nope.astype(jnp.float32), w_uk.astype(jnp.float32)).astype(jnp.bfloat16)
    query_vec = jnp.concatenate([q_lat, q_rot], axis=-1)
    lat_out = lax.map(lambda row_item: row_attention(row_item[0], row_item[1], row_item[2]), (query_vec, new_cache, lengths))
    head_out = jnp.einsum('bhk,hkv->bhv', lat_out.astype(jnp.float32), w_uv.astype(jnp.float32)).astype(jnp.bfloat16)
    attn_out = jnp.dot(head_out.reshape(BATCH, NUM_HEADS * V_DIM), w_o, preferred_element_type=jnp.float32)
    x_mid = (x_rows.astype(jnp.float32) + attn_out).astype(jnp.bfloat16)
    ffn_in = rms_norm(x_mid, ffn_g)
    hidden = (jax.nn.silu(jnp.dot(ffn_in, w_gate, preferred_element_type=jnp.float32)) * jnp.dot(ffn_in, w_up, preferred_element_type=jnp.float32)).astype(jnp.bfloat16)
    ffn_out = jnp.dot(hidden, w_down, preferred_element_type=jnp.float32)
    return (x_mid.astype(jnp.float32) + ffn_out).astype(jnp.bfloat16), new_cache


def draw_lengths(base_key):
    key_long, key_short, key_pick = jax.random.split(base_key, 3)
    long_len = jax.random.randint(key_long, (BATCH,), 0, SEQ_LEN)
    short_len = jax.random.randint(key_short, (BATCH,), 0, min(4, SEQ_LEN))
    pick_short = jax.random.randint(key_pick, (BATCH,), 0, 2)
    row_ids = jnp.arange(BATCH)
    drawn = jnp.where(pick_short == 1, short_len, long_len)
    drawn = jnp.where(row_ids == 0, SEQ_LEN - 1, drawn)
    drawn = jnp.where(row_ids == 1, 0, drawn)
    return drawn.astype(jnp.int32)


def draw_cache(base_key, lengths):
    key_common, key_noise = jax.random.split(base_key)
    common = jax.random.normal(key_common, (BATCH, 1, LAT_WIDTH), jnp.float32)
    slot_noise = jax.random.normal(key_noise, (BATCH, SEQ_LEN, LAT_WIDTH), jnp.float32)
    filled = (jnp.arange(SEQ_LEN)[None, :] < lengths[:, None])[:, :, None]
    return jnp.where(filled, 0.8 * common + 0.6 * slot_noise, 40.0 * slot_noise).astype(jnp.bfloat16)


def normal_weight(base_key, shape, fan_in):
    return (jax.random.normal(base_key, shape, jnp.float32) * fan_in ** -0.5).astype(jnp.bfloat16)


def setup_inputs(seed: int = 0, part: int = 0) -> dict:
    shared = jax.random.split(jax.random.key(seed), 13)
    part_keys = jax.random.split(jax.random.fold_in(jax.random.key(seed + 1), part), 4)
    lengths = draw_lengths(part_keys[1])
    return {
        'x': jax.random.normal(part_keys[0], (BATCH, MODEL_DIM), jnp.float32).astype(jnp.bfloat16),
        'lengths': lengths,
        'cache0': draw_cache(part_keys[2], lengths),
        'cache1': draw_cache(part_keys[3], lengths),
        'attn_gain': jax.random.uniform(shared[0], (LAYER_COUNT, MODEL_DIM), jnp.float32, 0.4, 1.6),
        'kv_gain': jax.random.uniform(shared[1], (LAYER_COUNT, KV_LORA), jnp.float32, 0.4, 1.6),
        'q_gain': jax.random.uniform(shared[2], (LAYER_COUNT, Q_LORA), jnp.float32, 0.4, 1.6),
        'ffn_gain': jax.random.uniform(shared[3], (LAYER_COUNT, MODEL_DIM), jnp.float32, 0.4, 1.6),
        'w_dkv': normal_weight(shared[4], (LAYER_COUNT, MODEL_DIM, LAT_WIDTH), MODEL_DIM),
        'w_qa': normal_weight(shared[5], (LAYER_COUNT, MODEL_DIM, Q_LORA), MODEL_DIM),
        'w_qb': normal_weight(shared[6], (LAYER_COUNT, Q_LORA, NUM_HEADS * QK_WIDTH), Q_LORA),
        'w_uk': normal_weight(shared[7], (LAYER_COUNT, NUM_HEADS, NOPE_DIM, KV_LORA), NOPE_DIM),
        'w_uv': normal_weight(shared[8], (LAYER_COUNT, NUM_HEADS, KV_LORA, V_DIM), KV_LORA),
        'w_o': normal_weight(shared[9], (LAYER_COUNT, NUM_HEADS * V_DIM, MODEL_DIM), NUM_HEADS * V_DIM),
        'w_gate': normal_weight(shared[10], (LAYER_COUNT, MODEL_DIM, FFN_DIM), MODEL_DIM),
        'w_up': normal_weight(shared[11], (LAYER_COUNT, MODEL_DIM, FFN_DIM), MODEL_DIM),
        'w_down': normal_weight(shared[12], (LAYER_COUNT, FFN_DIM, MODEL_DIM), FFN_DIM // 2),
    }


def reference(x, lengths, cache0, cache1, attn_gain, kv_gain, q_gain, ffn_gain, w_dkv, w_qa, w_qb, w_uk, w_uv, w_o, w_gate, w_up, w_down):
    cos_tab, sin_tab = rope_tables(lengths)
    caches = [cache0, cache1]
    new_caches = []
    x_rows = x
    for layer_idx in range(LAYER_COUNT):
        x_rows, new_cache = layer_step(x_rows, lengths, caches[layer_idx], cos_tab, sin_tab, attn_gain[layer_idx], kv_gain[layer_idx], q_gain[layer_idx], ffn_gain[layer_idx], w_dkv[layer_idx], w_qa[layer_idx], w_qb[layer_idx], w_uk[layer_idx], w_uv[layer_idx], w_o[layer_idx], w_gate[layer_idx], w_up[layer_idx], w_down[layer_idx])
        new_caches.append(new_cache)
    return (x_rows, new_caches[0], new_caches[1])
```

```python
import jax
import jax.numpy as jnp
from jax import lax
from jax.sharding import PartitionSpec as P

NORM_EPS = 1e-6
ROPE_BASE = 10000.0
F32 = jnp.float32
BF16 = jnp.bfloat16


def rms_norm(values, gain_vec):
    wide_vals = values.astype(F32)
    inv_rms = lax.rsqrt(jnp.mean(wide_vals * wide_vals, axis=-1, keepdims=True) + NORM_EPS)
    return (wide_vals * inv_rms * gain_vec).astype(BF16)


def rope_tables(lengths, rope_dim):
    half_dim = rope_dim // 2
    inv_freq = ROPE_BASE ** (-2.0 * jnp.arange(half_dim).astype(F32) / rope_dim)
    angles = lengths.astype(F32)[:, None] * inv_freq[None, :]
    return jnp.cos(angles), jnp.sin(angles)


def rotate(values, cos_tab, sin_tab):
    half_dim = values.shape[-1] // 2
    first_half = values[..., :half_dim]
    second_half = values[..., half_dim:]
    return jnp.concatenate([first_half * cos_tab - second_half * sin_tab, second_half * cos_tab + first_half * sin_tab], axis=-1)


def dot(a, b):
    return jnp.dot(a, b, preferred_element_type=F32)


def low_rank(x_rows, cos_tab, sin_tab, attn_g, kv_g, q_g, w_dkv, w_qa, latent):
    normed = rms_norm(x_rows, attn_g)
    kv_lat = dot(normed, w_dkv)
    entry = [rms_norm(kv_lat[:, :latent], kv_g), rotate(kv_lat[:, latent:], cos_tab, sin_tab).astype(BF16)]
    q_low = rms_norm(dot(normed, w_qa), q_g)
    return jnp.concatenate(entry + [q_low], axis=-1)


def attention(entry, q_low, lengths, cache, cos_tab, sin_tab, w_qb, w_uk, w_uv, w_o):
    row_count = entry.shape[0]
    head_count, nope_dim, latent = w_uk.shape
    qk_width = w_qb.shape[1] // head_count
    slot_ids = jnp.arange(cache.shape[1])
    is_slot = (slot_ids[None, :] == lengths[:, None])[:, :, None]
    new_cache = jnp.where(is_slot, entry[:, None, :], cache)
    q_full = dot(q_low, w_qb).reshape(row_count, head_count, qk_width)
    q_nope = q_full[:, :, :nope_dim].astype(BF16)
    q_rot = rotate(q_full[:, :, nope_dim:], cos_tab[:, None, :], sin_tab[:, None, :]).astype(BF16)
    q_lat = jnp.einsum('bhn,hnk->bhk', q_nope, w_uk, preferred_element_type=F32).astype(BF16)
    query_vec = jnp.concatenate([q_lat, q_rot], axis=-1)
    scores = jnp.einsum('bhk,btk->bht', query_vec, new_cache, preferred_element_type=F32) * qk_width ** -0.5
    valid_mask = (slot_ids[None, :] <= lengths[:, None])[:, None, :]
    att_probs = jax.nn.softmax(jnp.where(valid_mask, scores, -1e30), axis=-1).astype(BF16)
    lat_out = jnp.einsum('bht,btk->bhk', att_probs, new_cache, preferred_element_type=F32)[:, :, :latent].astype(BF16)
    head_out = jnp.einsum('cil,ilw->ciw', lat_out, w_uv, preferred_element_type=F32).astype(BF16)
    return dot(head_out.reshape(row_count, head_count * w_uv.shape[2]), w_o), new_cache


def solution(mesh):
    dp_size = mesh.shape['dp']
    row_spec = P(('rep', 'dp'), None)
    cache_spec = P(('rep', 'dp'), None, None)
    in_specs = (row_spec, P(('rep', 'dp')), cache_spec, cache_spec, P(), P(), P(), P(), P(), P(), P(None, None, 'tp'), P(None, 'tp', None, None), P(None, 'tp', None, None), P(None, 'tp', None), P(), P(), P())
    out_specs = (row_spec, cache_spec, cache_spec)
    tp_swap = [(0, 1), (1, 0)]
    core_swap = [(i, i ^ 1) for i in range(dp_size)]

    def local_step(x, lengths, cache0, cache1, attn_gain, kv_gain, q_gain, ffn_gain, w_dkv, w_qa, w_qb, w_uk, w_uv, w_o, w_gate, w_up, w_down):
        row_count, model_dim = x.shape
        half = row_count // 2
        latent = w_uk.shape[3]
        width = cache0.shape[2]
        tp = lax.axis_index('tp')
        core = lax.axis_index('dp') % 2
        ffn_width = w_gate.shape[2] // 2
        ffn_start = core * ffn_width
        cos_tab, sin_tab = rope_tables(lengths, width - latent)

        def own(a):
            return lax.dynamic_slice_in_dim(a, tp * half, half, 0)

        def gather_tp(mine):
            other = lax.ppermute(mine, 'tp', tp_swap)
            return jnp.where(tp == 0, jnp.concatenate([mine, other], 0), jnp.concatenate([other, mine], 0))

        new_caches = []
        x_own = own(x)
        for i, cache in enumerate((cache0, cache1)):
            args = (attn_gain[i], kv_gain[i], q_gain[i], w_dkv[i], w_qa[i], latent)
            if i == 0:
                low = low_rank(x, cos_tab, sin_tab, *args)
            else:
                low = gather_tp(low_rank(x_own, own(cos_tab), own(sin_tab), *args))
            part, new_cache = attention(low[:, :width], low[:, width:], lengths, cache, cos_tab, sin_tab, w_qb[i], w_uk[i], w_uv[i], w_o[i])
            theirs = lax.dynamic_slice_in_dim(part, (1 - tp) * half, half, 0)
            arrived = lax.ppermute(theirs, 'tp', tp_swap)
            x_mid = (x_own.astype(F32) + (own(part) + arrived)).astype(BF16)
            ffn_in = rms_norm(x_mid, ffn_gain[i])
            pair_in = jnp.concatenate([ffn_in, lax.ppermute(ffn_in, 'dp', core_swap)], 0)
            gate_cols = lax.dynamic_slice(w_gate, (i, 0, ffn_start), (1, model_dim, ffn_width))[0]
            up_cols = lax.dynamic_slice(w_up, (i, 0, ffn_start), (1, model_dim, ffn_width))[0]
            down_rows = lax.dynamic_slice(w_down, (i, ffn_start, 0), (1, ffn_width, model_dim))[0]
            hidden = (jax.nn.silu(dot(pair_in, gate_cols)) * dot(pair_in, up_cols)).astype(BF16)
            partial = dot(hidden, down_rows).astype(BF16)
            back = lax.ppermute(partial[half:], 'dp', core_swap)
            x_own = (x_mid.astype(F32) + (partial[:half].astype(F32) + back.astype(F32))).astype(BF16)
            new_caches.append(new_cache)
        return gather_tp(x_own), new_caches[0], new_caches[1]

    return jax.shard_map(local_step, mesh=mesh, in_specs=in_specs, out_specs=out_specs, check_vma=False)
```

```python
import functools

import jax
import jax.numpy as jnp
from jax import lax
from jax.experimental import pallas as pl
from jax.experimental.pallas import tpu as pltpu
from jax.sharding import PartitionSpec as P

NORM_EPS = 1e-6
ROPE_BASE = 10000.0
F32 = jnp.float32
BF16 = jnp.bfloat16
ROWS_PER_STEP = 8
SLOTS = 12
AHEAD = 8
LANES = 128
PITCH_PAD = 8
HIDDEN_BLOCKS = 5
HIDDEN_SLOTS = 3
OUT_BLOCKS = 5
MESH = pl.DeviceIdType.MESH
VMEM_LIMIT = 60 * 1024 * 1024


def rms_norm(values, gain_vec):
    wide_vals = values.astype(F32)
    inv_rms = lax.rsqrt(jnp.mean(wide_vals * wide_vals, axis=-1, keepdims=True) + NORM_EPS)
    return (wide_vals * inv_rms * gain_vec).astype(BF16)


def rope_tables(lengths, rope_dim):
    half_dim = rope_dim // 2
    inv_freq = ROPE_BASE ** (-2.0 * jnp.arange(half_dim).astype(F32) / rope_dim)
    angles = lengths.astype(F32)[:, None] * inv_freq[None, :]
    cos_tab, sin_tab = jnp.cos(angles), jnp.sin(angles)
    return jnp.concatenate([cos_tab, cos_tab], axis=1), jnp.concatenate([-sin_tab, sin_tab], axis=1)


def rotate(turn, cos2, sin2):
    half = turn.shape[1] // 2
    swapped = jnp.concatenate([turn[:, half:], turn[:, :half]], axis=1)
    return turn * cos2 + swapped * sin2


def dot(a, b):
    return jnp.dot(a, b, preferred_element_type=F32)


def dot_nt(a, b):
    return lax.dot_general(a, b, (((1,), (1,)), ((), ())), preferred_element_type=F32)


def low_rank(x_rows, cos2, sin2, attn_g, kv_g, q_g, dkv, qa, out):
    q_rank = qa.shape[1]
    latent = kv_g.shape[1]
    width = dkv.shape[0]
    rows = x_rows.shape[0]
    normed = rms_norm(x_rows, attn_g)
    out[:, 0:q_rank] = rms_norm(dot(normed, qa[...]), q_g)
    kv_lat = dot_nt(normed, dkv[...])
    out[:, q_rank:q_rank + latent] = rms_norm(kv_lat[:, :latent], kv_g)
    turned = rotate(kv_lat[:, latent:], cos2, sin2).astype(BF16)
    pad = jnp.zeros((rows, out.shape[1] - q_rank - width), BF16)
    out[:, q_rank + latent:] = jnp.concatenate([turned, pad], axis=1)


def attention_kernel(layer, heads, nope, latent, lengths, given, cos_ref, sin_ref, attn_g, kv_g, q_g, cache, w_dkv, w_qa, w_qb, w_uk, w_uv, w_o, part, new_cache,
                     blocks, low, dkv, qa, qb, uk, uv, wo, entry, q_lat, q_rot, o_lat, o_cat, wsem, rsem, ssem):
    rows = cos_ref.shape[0]
    pitch = rows + PITCH_PAD
    slots = cache.shape[2]
    width = cache.shape[1]
    rope = width - latent
    qk = nope + rope
    q_rank = qb.shape[0]
    steps = rows // ROWS_PER_STEP
    weights = [(w_dkv, dkv), (w_qa, qa), (w_qb, qb), (w_uk, uk), (w_uv, uv), (w_o, wo)]

    def load_weight(n):
        return pltpu.make_async_copy(weights[n][0].at[layer], weights[n][1], wsem.at[n])

    def row_slice(step):
        return pl.ds(pl.multiple_of(step * ROWS_PER_STEP, ROWS_PER_STEP), ROWS_PER_STEP)

    def load(step, slot):
        return pltpu.make_async_copy(cache.at[row_slice(step)], blocks.at[slot], rsem.at[slot])

    def store(step, slot):
        return pltpu.make_async_copy(blocks.at[slot], new_cache.at[row_slice(step)], ssem.at[slot])

    first = layer == 0
    for n in ((0, 1) if first else ()) + (2, 3):
        load_weight(n).start()
    for step in range(AHEAD):
        load(step, step).start()
    load_weight(4).start()
    load_weight(5).start()

    cos2 = cos_ref[...]
    sin2 = sin_ref[...]
    if first:
        load_weight(0).wait()
        load_weight(1).wait()
        low_rank(given[...], cos2, sin2, attn_g[layer:layer + 1], kv_g[layer:layer + 1], q_g[layer:layer + 1], dkv, qa, low)
    else:
        low = given
    entry[...] = low[:, q_rank:].astype(F32)
    load_weight(2).wait()
    load_weight(3).wait()
    group = 4
    for g in range(heads // group):
        q_part = dot(low[:, :q_rank], qb[:, g * group * qk:(g + 1) * group * qk])
        for j in range(group):
            h = g * group + j
            mine = q_part[:, j * qk:(j + 1) * qk]
            q_rot[h * pitch:h * pitch + rows, 0:rope] = rotate(mine[:, nope:], cos2, sin2)
            latent_q = dot(mine[:, :nope].astype(BF16), uk[h])
            for c in range(latent // LANES):
                q_lat[c, h * pitch:h * pitch + rows, :] = latent_q[:, c * LANES:(c + 1) * LANES]

    scale = qk ** -0.5
    lane = lax.broadcasted_iota(jnp.int32, (1, slots), 1)

    def one_step(step, carry):
        slot = lax.rem(step, SLOTS)
        load(step, slot).wait()
        columns = jnp.transpose(entry[row_slice(step), :])
        probs = []
        for r in range(ROWS_PER_STEP):
            row = step * ROWS_PER_STEP + r
            length = lengths[row]
            fresh = jnp.broadcast_to(columns[:width, r:r + 1], (width, slots)).astype(BF16)
            blocks[slot, r] = jnp.where(lane == length, fresh, blocks[slot, r])
            lat = jnp.concatenate([q_lat.at[c][pl.ds(row, heads, stride=pitch), :] for c in range(latent // LANES)], axis=1).astype(BF16)
            rot = q_rot[pl.ds(row, heads, stride=pitch), :][:, :rope].astype(BF16)
            score = dot(lat, blocks[slot, r, :latent]) + dot(rot, blocks[slot, r, latent:])
            score = jnp.where(lane <= length, score * scale, -1e30)
            score = jnp.exp(score - jnp.max(score, axis=1, keepdims=True))
            probs.append((score * (1.0 / jnp.sum(score, axis=1, keepdims=True))).astype(BF16))
        for r in range(ROWS_PER_STEP):
            row = step * ROWS_PER_STEP + r
            mixed = dot_nt(probs[r], blocks[slot, r, :latent])
            for c in range(latent // LANES):
                o_lat.at[c][pl.ds(row, heads, stride=pitch), :] = mixed[:, c * LANES:(c + 1) * LANES]
        store(step, slot).start()

        @pl.when(step + AHEAD < steps)
        def _():
            @pl.when(step + AHEAD >= SLOTS)
            def _():
                store(step + AHEAD - SLOTS, lax.rem(step + AHEAD, SLOTS)).wait()
            load(step + AHEAD, lax.rem(step + AHEAD, SLOTS)).start()
        return carry

    lax.fori_loop(0, steps, one_step, 0)
    load_weight(4).wait()
    load_weight(5).wait()
    for h in range(0, heads, 2):
        pair = []
        for n in (h, h + 1):
            mixed = jnp.concatenate([o_lat[c, n * pitch:n * pitch + rows, :] for c in range(latent // LANES)], axis=1)
            pair.append(dot_nt(mixed.astype(BF16), uv[n]).astype(BF16))
        v = uv.shape[1]
        o_cat[:, h * v:(h + 2) * v] = jnp.concatenate(pair, axis=1)
    chunk = 512
    for n in range(wo.shape[1] // chunk):
        part[:, n * chunk:(n + 1) * chunk] = dot(o_cat[...], wo[:, n * chunk:(n + 1) * chunk])
    for step in range(max(steps - SLOTS, 0), steps):
        store(step, step % SLOTS).wait()


ANY = pl.BlockSpec(memory_space=pl.ANY)
VMEM = pl.BlockSpec(memory_space=pltpu.VMEM)
SMEM = pl.BlockSpec(memory_space=pltpu.SMEM)


def low_width(w_qa, w_dkv_t):
    return -(-(w_qa.shape[2] + w_dkv_t.shape[1]) // LANES) * LANES


def attention(layer, given, lengths, cache_t, cos2, sin2, gains, w_dkv_t, w_qa, w_qb, w_uk, w_uv_t, w_o):
    rows = lengths.shape[0]
    _, heads, nope, latent = w_uk.shape
    width, slots = cache_t.shape[1:]
    model = w_o.shape[2]
    padded = low_width(w_qa, w_dkv_t)
    q_rank = w_qa.shape[2]
    low_shapes = [((rows, padded), BF16), (w_dkv_t.shape[1:], BF16), (w_qa.shape[1:], BF16)]
    if layer:
        low_shapes = [((8, LANES), BF16)] * 3
    return pl.pallas_call(
        functools.partial(attention_kernel, layer, heads, nope, latent),
        out_shape=(jax.ShapeDtypeStruct((rows, model), F32), jax.ShapeDtypeStruct(cache_t.shape, BF16)),
        in_specs=[SMEM] + [VMEM] * 6 + [ANY] * 7,
        out_specs=(VMEM, ANY),
        scratch_shapes=[pltpu.VMEM((SLOTS, ROWS_PER_STEP, width, slots), BF16)] + [pltpu.VMEM(*s) for s in low_shapes] + [
            pltpu.VMEM(w_qb.shape[1:], BF16),
            pltpu.VMEM(w_uk.shape[1:], BF16),
            pltpu.VMEM(w_uv_t.shape[1:], BF16),
            pltpu.VMEM(w_o.shape[1:], BF16),
            pltpu.VMEM((rows, padded - q_rank), F32),
            pltpu.VMEM((latent // LANES, heads * (rows + PITCH_PAD), LANES), F32),
            pltpu.VMEM((heads * (rows + PITCH_PAD), LANES), F32),
            pltpu.VMEM((latent // LANES, heads * (rows + PITCH_PAD), LANES), F32),
            pltpu.VMEM((rows, w_o.shape[1]), BF16),
            pltpu.SemaphoreType.DMA((6,)),
            pltpu.SemaphoreType.DMA((SLOTS,)),
            pltpu.SemaphoreType.DMA((SLOTS,)),
        ],
        compiler_params=pltpu.CompilerParams(vmem_limit_bytes=VMEM_LIMIT),
        name="attention",
    )(lengths, given, cos2, sin2, *gains, cache_t, w_dkv_t, w_qa, w_qb, w_uk, w_uv_t, w_o)


def ffn_kernel(layer, last, part, x_in, cos_ref, sin_ref, ffn_g, attn_g, kv_g, q_g, w_gate, w_up, w_down, w_dkv, w_qa, *rest):
    if last:
        out, *rest = rest
        gates, ups, downs, arrived, x_mid, g_pair, hidden, mine, outgoing, incoming, x_new, x_far, sems, dsem, ssem, rsem = rest
    else:
        low_out, x_out, *rest = rest
        gates, ups, downs, arrived, x_mid, g_pair, hidden, mine, outgoing, incoming, low_mine, low_far, dkv, qa, sems, dsem, lsem, ssem, rsem = rest
    tp = lax.axis_index("tp")
    dp = lax.axis_index("dp")
    core = lax.rem(dp, 2)
    peer = {"tp": 1 - tp}
    mate = {"dp": dp + 1 - 2 * core}
    half, model = arrived.shape
    h_block = gates.shape[2]
    h_width = hidden.shape[1]
    o_block = downs.shape[2]
    own = pl.ds(pl.multiple_of(tp * half, half), half)
    far = pl.ds(pl.multiple_of((1 - tp) * half, half), half)

    def hidden_loads(b, slot):
        cols = pl.ds(pl.multiple_of(core * h_width + b * h_block, LANES), h_block)
        return [pltpu.make_async_copy(w.at[layer, :, cols], v.at[slot], sems.at[n, slot]) for n, (w, v) in enumerate(((w_gate, gates), (w_up, ups)))]

    def down_load(c):
        return pltpu.make_async_copy(w_down.at[layer, pl.ds(pl.multiple_of(core * h_width, LANES), h_width), pl.ds(c * o_block, o_block)], downs.at[c], dsem.at[c])

    for b in range(HIDDEN_SLOTS):
        for copy in hidden_loads(b, b):
            copy.start()
    for c in range(OUT_BLOCKS):
        down_load(c).start()
    if not last:
        loads = [pltpu.make_async_copy(w_dkv.at[layer + 1], dkv, lsem.at[0]), pltpu.make_async_copy(w_qa.at[layer + 1], qa, lsem.at[1])]
        for copy in loads:
            copy.start()

    barrier = pltpu.get_barrier_semaphore()
    for other in (peer, mate):
        pl.semaphore_signal(barrier, inc=1, device_id=other, device_id_type=MESH)
    pl.semaphore_wait(barrier, 2)

    def send(src, dst, n, to):
        return pltpu.make_async_remote_copy(src_ref=src, dst_ref=dst, send_sem=ssem.at[n], recv_sem=rsem.at[n], device_id=to, device_id_type=MESH)

    scatter = send(part.at[far], arrived, 0, peer)
    scatter.start()
    x_own = x_in[own, :] if layer == 0 else x_in[...]
    scatter.wait_recv()
    x_mid[...] = (x_own.astype(F32) + (part[own, :] + arrived[...])).astype(BF16)
    g_pair[0:half, :] = rms_norm(x_mid[...], ffn_g[layer:layer + 1])
    swap = send(g_pair.at[0:half], g_pair.at[half:2 * half], 1, mate)
    swap.start()
    swap.wait_recv()

    def hidden_step(b, carry):
        slot = lax.rem(b, HIDDEN_SLOTS)
        for copy in hidden_loads(b, slot):
            copy.wait()
        gate = dot(g_pair[...], gates[slot])
        up = dot(g_pair[...], ups[slot])
        hidden[:, pl.ds(pl.multiple_of(b * h_block, LANES), h_block)] = (jax.nn.silu(gate) * up).astype(BF16)

        @pl.when(b + HIDDEN_SLOTS < HIDDEN_BLOCKS)
        def _():
            for copy in hidden_loads(b + HIDDEN_SLOTS, slot):
                copy.start()
        return carry

    lax.fori_loop(0, HIDDEN_BLOCKS, hidden_step, 0)

    returns = [send(outgoing.at[c], incoming.at[c], 2 + c, mate) for c in range(OUT_BLOCKS)]
    if last:
        spreads = [send(x_new.at[c], x_far.at[c], 2 + OUT_BLOCKS + c, peer) for c in range(OUT_BLOCKS)]

    def finish(c):
        returns[c].wait_recv()
        cols = slice(c * o_block, (c + 1) * o_block)
        fresh = (x_mid[:, cols].astype(F32) + (mine[:, cols] + incoming[c].astype(F32))).astype(BF16)
        if last:
            x_new[c] = fresh
            spreads[c].start()
            out[own, cols] = fresh
        else:
            x_out[:, cols] = fresh

    for c in range(OUT_BLOCKS):
        down_load(c).wait()
        y = dot(hidden[...], downs[c])
        outgoing[c] = y[half:].astype(BF16)
        returns[c].start()
        mine[:, c * o_block:(c + 1) * o_block] = y[:half]
        if c:
            finish(c - 1)
    finish(OUT_BLOCKS - 1)

    if last:
        for c in range(OUT_BLOCKS):
            spreads[c].wait_recv()
            out[far, c * o_block:(c + 1) * o_block] = x_far[c]
            spreads[c].wait_send()
    else:
        for copy in loads:
            copy.wait()
        nxt = layer + 1
        low_rank(x_out[...], cos_ref[own, :], sin_ref[own, :], attn_g[nxt:nxt + 1], kv_g[nxt:nxt + 1], q_g[nxt:nxt + 1], dkv, qa, low_mine)
        share = send(low_mine, low_far, 2 + OUT_BLOCKS, peer)
        share.start()
        low_out[own, :] = low_mine[...]
        share.wait_recv()
        low_out[far, :] = low_far[...]
        share.wait_send()
    scatter.wait_send()
    swap.wait_send()
    for c in range(OUT_BLOCKS):
        returns[c].wait_send()


def ffn(layer, last, part, x_in, cos2, sin2, ffn_gain, gains, w_gate, w_up, w_down, w_dkv_t, w_qa):
    rows, model = part.shape
    half = rows // 2
    h_width = w_gate.shape[2] // 2
    h_block = h_width // HIDDEN_BLOCKS
    o_block = model // OUT_BLOCKS
    padded = low_width(w_qa, w_dkv_t)
    scratch = [
        pltpu.VMEM((HIDDEN_SLOTS, model, h_block), BF16),
        pltpu.VMEM((HIDDEN_SLOTS, model, h_block), BF16),
        pltpu.VMEM((OUT_BLOCKS, h_width, o_block), BF16),
        pltpu.VMEM((half, model), F32),
        pltpu.VMEM((half, model), BF16),
        pltpu.VMEM((rows, model), BF16),
        pltpu.VMEM((rows, h_width), BF16),
        pltpu.VMEM((half, model), F32),
        pltpu.VMEM((OUT_BLOCKS, half, o_block), BF16),
        pltpu.VMEM((OUT_BLOCKS, half, o_block), BF16),
    ]
    dma = pltpu.SemaphoreType.DMA
    if last:
        out_shape = jax.ShapeDtypeStruct((rows, model), BF16)
        out_specs = VMEM
        scratch += [pltpu.VMEM((OUT_BLOCKS, half, o_block), BF16)] * 2 + [dma((2, HIDDEN_SLOTS)), dma((OUT_BLOCKS,))]
    else:
        out_shape = (jax.ShapeDtypeStruct((rows, padded), BF16), jax.ShapeDtypeStruct((half, model), BF16))
        out_specs = (VMEM, VMEM)
        scratch += [pltpu.VMEM((half, padded), BF16)] * 2 + [pltpu.VMEM(w_dkv_t.shape[1:], BF16), pltpu.VMEM(w_qa.shape[1:], BF16)]
        scratch += [dma((2, HIDDEN_SLOTS)), dma((OUT_BLOCKS,)), dma((2,))]
    copies = 2 + OUT_BLOCKS + (OUT_BLOCKS if last else 1)
    return pl.pallas_call(
        functools.partial(ffn_kernel, layer, last),
        out_shape=out_shape,
        in_specs=[VMEM] * 8 + [ANY] * 5,
        out_specs=out_specs,
        scratch_shapes=scratch + [dma((copies,)), dma((copies,))],
        compiler_params=pltpu.CompilerParams(vmem_limit_bytes=VMEM_LIMIT, collective_id=layer, has_side_effects=True),
        name="ffn",
    )(part, x_in, cos2, sin2, ffn_gain, *gains, w_gate, w_up, w_down, w_dkv_t, w_qa)


def solution(mesh):
    row_spec = P(('rep', 'dp'), None)
    cache_spec = P(('rep', 'dp'), None, None)
    in_specs = (row_spec, P(('rep', 'dp')), cache_spec, cache_spec, P(), P(), P(), P(), P(), P(), P(None, None, 'tp'), P(None, 'tp', None, None), P(None, 'tp', None, None), P(None, 'tp', None), P(), P(), P())
    out_specs = (row_spec, cache_spec, cache_spec)

    def local_step(x, lengths, cache0, cache1, attn_gain, kv_gain, q_gain, ffn_gain, w_dkv, w_qa, w_qb, w_uk, w_uv, w_o, w_gate, w_up, w_down):
        cos2, sin2 = rope_tables(lengths, cache0.shape[2] - w_uk.shape[3])
        w_uv_t = jnp.swapaxes(w_uv, 2, 3)
        w_dkv_t = jnp.swapaxes(w_dkv, 1, 2)
        gains = (attn_gain, kv_gain, q_gain)
        caches = (cache0, cache1)
        given = x
        new_caches = []
        for i, cache in enumerate(caches):
            part, new_cache = attention(i, given, lengths, jnp.swapaxes(cache, 1, 2), cos2, sin2, gains, w_dkv_t, w_qa, w_qb, w_uk, w_uv_t, w_o)
            new_caches.append(jnp.swapaxes(new_cache, 1, 2))
            last = i == len(caches) - 1
            result = ffn(i, last, part, x, cos2, sin2, ffn_gain, gains, w_gate, w_up, w_down, w_dkv_t, w_qa)
            if not last:
                given, x = result
        return result, new_caches[0], new_caches[1]

    return jax.shard_map(local_step, mesh=mesh, in_specs=in_specs, out_specs=out_specs, check_vma=False)
```

```python
import functools

import jax
import jax.numpy as jnp
from jax import lax
from jax.experimental import pallas as pl
from jax.experimental.pallas import tpu as pltpu
from jax.sharding import PartitionSpec as P

NORM_EPS = 1e-6
ROPE_BASE = 10000.0
F32 = jnp.float32
BF16 = jnp.bfloat16
ROWS_PER_STEP = 16
SLOTS = 5
OUT_SLOTS = 3
LANES = 128
PITCH_PAD = 8
HIDDEN_BLOCKS = 5
HIDDEN_SLOTS = 3
OUT_BLOCKS = 5
MESH = pl.DeviceIdType.MESH
VMEM_LIMIT = 60 * 1024 * 1024


def rms_norm(values, gain_vec):
    wide_vals = values.astype(F32)
    inv_rms = lax.rsqrt(jnp.mean(wide_vals * wide_vals, axis=-1, keepdims=True) + NORM_EPS)
    return (wide_vals * inv_rms * gain_vec).astype(BF16)


def rope_tables(lengths, rope_dim):
    half_dim = rope_dim // 2
    lane = jnp.arange(LANES)
    inv_freq = ROPE_BASE ** (-2.0 * (lane % half_dim).astype(F32) / rope_dim)
    angles = lengths.astype(F32)[:, None] * inv_freq[None, :]
    sines = jnp.sin(angles)
    return jnp.where(lane < rope_dim, jnp.cos(angles), jnp.where(lane % rope_dim < half_dim, -sines, sines))


def rotate(turn, table):
    half = turn.shape[1] // 2
    swapped = jnp.concatenate([turn[:, half:], turn[:, :half]], axis=1)
    return turn * table[:, :2 * half] + swapped * table[:, 2 * half:4 * half]


def dot(a, b):
    return jnp.dot(a, b, preferred_element_type=F32)


def dot_nt(a, b):
    return lax.dot_general(a, b, (((1,), (1,)), ((), ())), preferred_element_type=F32)


def low_rank(x_rows, table, attn_g, kv_g, q_g, dkv, qa, out):
    q_rank = qa.shape[1]
    latent = kv_g.shape[1]
    width = dkv.shape[0]
    rows = x_rows.shape[0]
    normed = rms_norm(x_rows, attn_g)
    out[:, 0:q_rank] = rms_norm(dot(normed, qa[...]), q_g)
    kv_lat = dot_nt(normed, dkv[...])
    out[:, q_rank:q_rank + latent] = rms_norm(kv_lat[:, :latent], kv_g)
    turned = rotate(kv_lat[:, latent:], table).astype(BF16)
    pad = jnp.zeros((rows, out.shape[1] - q_rank - width), BF16)
    out[:, q_rank + latent:] = jnp.concatenate([turned, pad], axis=1)


def attention_kernel(layer, heads, nope, latent, lengths, given, table_ref, attn_g, kv_g, q_g, cache, w_dkv, w_qa, w_qb, w_uk, w_uv, w_o, part, new_cache,
                     blocks, outs, low, dkv, qa, qb, uk, uv, wo, entry, q_lat, q_rot, o_lat, o_cat, wsem, rsem, ssem):
    rows = table_ref.shape[0]
    pitch = rows + PITCH_PAD
    slots = cache.shape[2]
    width = cache.shape[1]
    rope = width - latent
    qk = nope + rope
    q_rank = qb.shape[0]
    steps = rows // ROWS_PER_STEP
    weights = [(w_dkv, dkv), (w_qa, qa), (w_qb, qb), (w_uk, uk), (w_uv, uv), (w_o, wo)]

    def load_weight(n):
        return pltpu.make_async_copy(weights[n][0].at[layer], weights[n][1], wsem.at[n])

    def row_slice(step):
        return pl.ds(pl.multiple_of(step * ROWS_PER_STEP, ROWS_PER_STEP), ROWS_PER_STEP)

    def load(step, slot):
        return pltpu.make_async_copy(cache.at[row_slice(step)], blocks.at[slot], rsem.at[slot])

    def store(step, slot):
        return pltpu.make_async_copy(outs.at[slot], new_cache.at[row_slice(step)], ssem.at[slot])

    first = layer == 0
    for n in ((0, 1) if first else ()) + (2, 3):
        load_weight(n).start()
    for step in range(SLOTS):
        load(step, step).start()
    load_weight(4).start()
    load_weight(5).start()

    table = table_ref[...]
    if first:
        load_weight(0).wait()
        load_weight(1).wait()
        low_rank(given[...], table, attn_g[layer:layer + 1], kv_g[layer:layer + 1], q_g[layer:layer + 1], dkv, qa, low)
    else:
        low = given
    entry[...] = low[:, q_rank:].astype(F32)
    load_weight(2).wait()
    load_weight(3).wait()
    group = 4
    for g in range(heads // group):
        q_part = dot(low[:, :q_rank], qb[:, g * group * qk:(g + 1) * group * qk])
        for j in range(group):
            h = g * group + j
            mine = q_part[:, j * qk:(j + 1) * qk]
            q_rot[h * pitch:h * pitch + rows, :] = jnp.concatenate([rotate(mine[:, nope:], table).astype(BF16).astype(F32), jnp.zeros((rows, LANES - rope), F32)], axis=1)
            latent_q = dot(mine[:, :nope].astype(BF16), uk[h])
            for c in range(latent // LANES):
                q_lat[c, h * pitch:h * pitch + rows, :] = latent_q[:, c * LANES:(c + 1) * LANES].astype(BF16).astype(F32)

    scale = qk ** -0.5
    lane = lax.broadcasted_iota(jnp.int32, (1, slots), 1)

    def one_step(step, carry):
        slot = lax.rem(step, SLOTS)
        load(step, slot).wait()
        drain = lax.rem(step, OUT_SLOTS)

        @pl.when(step >= OUT_SLOTS)
        def _():
            store(step - OUT_SLOTS, drain).wait()

        fresh_rows = entry[row_slice(step), :]
        columns = jnp.transpose(fresh_rows)
        scores, probs, news = [], [], []
        for r in range(ROWS_PER_STEP):
            row = step * ROWS_PER_STEP + r
            lat = jnp.concatenate([q_lat.at[c][pl.ds(row, heads, stride=pitch), :] for c in range(latent // LANES)], axis=1)
            rot = q_rot[pl.ds(row, heads, stride=pitch), :]
            new_score = lat * fresh_rows[r:r + 1, :latent]
            new_score = jnp.sum(new_score[:, :LANES] + new_score[:, LANES:] + rot * fresh_rows[r:r + 1, latent:], axis=1, keepdims=True)
            score = dot(lat.astype(BF16), blocks[slot, r, :latent]) + dot(rot[:, :rope].astype(BF16), blocks[slot, r, latent:])
            scores.append(score)
            news.append(new_score)
        for r in range(ROWS_PER_STEP):
            length = lengths[step * ROWS_PER_STEP + r]
            new_score = news[r] * scale
            score = jnp.where(lane < length, scores[r] * scale, -1e30)
            top = jnp.maximum(jnp.max(score, axis=1, keepdims=True), new_score)
            score = jnp.exp(score - top)
            new_score = jnp.exp(new_score - top)
            inverse = 1.0 / (jnp.sum(score, axis=1, keepdims=True) + new_score)
            probs.append((score * inverse).astype(BF16))
            news[r] = (new_score * inverse).astype(BF16).astype(F32)
        for r in range(ROWS_PER_STEP):
            row = step * ROWS_PER_STEP + r
            mixed = dot_nt(probs[r], blocks[slot, r, :latent]) + news[r] * fresh_rows[r:r + 1, :latent]
            for c in range(latent // LANES):
                o_lat.at[c][pl.ds(row, heads, stride=pitch), :] = mixed[:, c * LANES:(c + 1) * LANES]
        for r in range(ROWS_PER_STEP):
            length = lengths[step * ROWS_PER_STEP + r]
            fresh = jnp.broadcast_to(columns[:width, r:r + 1], (width, slots)).astype(BF16)
            outs[drain, r] = jnp.where(lane == length, fresh, blocks[slot, r])
        store(step, drain).start()

        @pl.when(step + SLOTS < steps)
        def _():
            load(step + SLOTS, slot).start()
        return carry

    lax.fori_loop(0, steps, one_step, 0)
    load_weight(4).wait()
    load_weight(5).wait()
    for h in range(0, heads, 2):
        pair = []
        for n in (h, h + 1):
            mixed = jnp.concatenate([o_lat[c, n * pitch:n * pitch + rows, :] for c in range(latent // LANES)], axis=1)
            pair.append(dot_nt(mixed.astype(BF16), uv[n]).astype(BF16))
        v = uv.shape[1]
        o_cat[:, h * v:(h + 2) * v] = jnp.concatenate(pair, axis=1)
    chunk = 512
    for n in range(wo.shape[1] // chunk):
        part[:, n * chunk:(n + 1) * chunk] = dot(o_cat[...], wo[:, n * chunk:(n + 1) * chunk])
    for step in range(max(steps - OUT_SLOTS, 0), steps):
        store(step, step % OUT_SLOTS).wait()


ANY = pl.BlockSpec(memory_space=pl.ANY)
VMEM = pl.BlockSpec(memory_space=pltpu.VMEM)
SMEM = pl.BlockSpec(memory_space=pltpu.SMEM)


def low_width(w_qa, w_dkv_t):
    return -(-(w_qa.shape[2] + w_dkv_t.shape[1]) // LANES) * LANES


def attention(layer, given, lengths, cache_t, table, gains, w_dkv_t, w_qa, w_qb, w_uk, w_uv_t, w_o):
    rows = lengths.shape[0]
    _, heads, nope, latent = w_uk.shape
    width, slots = cache_t.shape[1:]
    model = w_o.shape[2]
    padded = low_width(w_qa, w_dkv_t)
    q_rank = w_qa.shape[2]
    low_shapes = [((rows, padded), BF16), (w_dkv_t.shape[1:], BF16), (w_qa.shape[1:], BF16)]
    if layer:
        low_shapes = [((8, LANES), BF16)] * 3
    return pl.pallas_call(
        functools.partial(attention_kernel, layer, heads, nope, latent),
        out_shape=(jax.ShapeDtypeStruct((rows, model), F32), jax.ShapeDtypeStruct(cache_t.shape, BF16)),
        in_specs=[SMEM] + [VMEM] * 5 + [ANY] * 7,
        out_specs=(VMEM, ANY),
        scratch_shapes=[pltpu.VMEM((n, ROWS_PER_STEP, width, slots), BF16) for n in (SLOTS, OUT_SLOTS)] + [pltpu.VMEM(*s) for s in low_shapes] + [
            pltpu.VMEM(w_qb.shape[1:], BF16),
            pltpu.VMEM(w_uk.shape[1:], BF16),
            pltpu.VMEM(w_uv_t.shape[1:], BF16),
            pltpu.VMEM(w_o.shape[1:], BF16),
            pltpu.VMEM((rows, padded - q_rank), F32),
            pltpu.VMEM((latent // LANES, heads * (rows + PITCH_PAD), LANES), F32),
            pltpu.VMEM((heads * (rows + PITCH_PAD), LANES), F32),
            pltpu.VMEM((latent // LANES, heads * (rows + PITCH_PAD), LANES), F32),
            pltpu.VMEM((rows, w_o.shape[1]), BF16),
            pltpu.SemaphoreType.DMA((6,)),
            pltpu.SemaphoreType.DMA((SLOTS,)),
            pltpu.SemaphoreType.DMA((OUT_SLOTS,)),
        ],
        compiler_params=pltpu.CompilerParams(vmem_limit_bytes=VMEM_LIMIT),
        name="attention",
    )(lengths, given, table, *gains, cache_t, w_dkv_t, w_qa, w_qb, w_uk, w_uv_t, w_o)


def ffn_kernel(layer, last, part, x_in, table_ref, ffn_g, attn_g, kv_g, q_g, w_gate, w_up, w_down, w_dkv, w_qa, *rest):
    if last:
        out_own, out_far, *rest = rest
        wides, downs, arrived, x_mid, g_pair, hidden, mine, outgoing, incoming, x_new, x_far, sems, dsem, ssem, rsem = rest
    else:
        low_out, x_out, *rest = rest
        wides, downs, arrived, x_mid, g_pair, hidden, mine, outgoing, incoming, low_mine, low_far, dkv, qa, sems, dsem, lsem, ssem, rsem = rest
    tp = lax.axis_index("tp")
    dp = lax.axis_index("dp")
    core = lax.rem(dp, 2)
    peer = {"tp": 1 - tp}
    mate = {"dp": dp + 1 - 2 * core}
    half, model = arrived.shape
    h_block = wides.shape[2] // 2
    h_width = hidden.shape[1]
    o_block = downs.shape[2]
    own = pl.ds(pl.multiple_of(tp * half, half), half)
    far = pl.ds(pl.multiple_of((1 - tp) * half, half), half)

    def hidden_loads(b, slot):
        cols = pl.ds(pl.multiple_of(core * h_width + b * h_block, LANES), h_block)
        return [pltpu.make_async_copy(w.at[layer, :, cols], wides.at[slot, :, pl.ds(n * h_block, h_block)], sems.at[n, slot]) for n, w in enumerate((w_gate, w_up))]

    def down_load(c):
        return pltpu.make_async_copy(w_down.at[layer, pl.ds(pl.multiple_of(core * h_width, LANES), h_width), pl.ds(c * o_block, o_block)], downs.at[c], dsem.at[c])

    for b in range(HIDDEN_SLOTS):
        for copy in hidden_loads(b, b):
            copy.start()
    for c in range(OUT_BLOCKS):
        down_load(c).start()
    if not last:
        loads = [pltpu.make_async_copy(w_dkv.at[layer + 1], dkv, lsem.at[0]), pltpu.make_async_copy(w_qa.at[layer + 1], qa, lsem.at[1])]
        for copy in loads:
            copy.start()

    barrier = pltpu.get_barrier_semaphore()
    for other in (peer, mate):
        pl.semaphore_signal(barrier, inc=1, device_id=other, device_id_type=MESH)
    pl.semaphore_wait(barrier, 2)

    def send(src, dst, n, to):
        return pltpu.make_async_remote_copy(src_ref=src, dst_ref=dst, send_sem=ssem.at[n], recv_sem=rsem.at[n], device_id=to, device_id_type=MESH)

    scatter = send(part.at[far], arrived, 0, peer)
    scatter.start()
    x_own = x_in[own, :] if layer == 0 else x_in[...]
    scatter.wait_recv()
    x_mid[...] = (x_own.astype(F32) + (part[own, :] + arrived[...])).astype(BF16)
    g_pair[0:half, :] = rms_norm(x_mid[...], ffn_g[layer:layer + 1])
    swap = send(g_pair.at[0:half], g_pair.at[half:2 * half], 1, mate)
    swap.start()
    swap.wait_recv()

    def hidden_step(b, carry):
        slot = lax.rem(b, HIDDEN_SLOTS)
        for copy in hidden_loads(b, slot):
            copy.wait()
        both = dot(g_pair[...], wides[slot])
        gate, up = both[:, :h_block], both[:, h_block:]
        hidden[:, pl.ds(pl.multiple_of(b * h_block, LANES), h_block)] = (jax.nn.silu(gate) * up).astype(BF16)

        @pl.when(b + HIDDEN_SLOTS < HIDDEN_BLOCKS)
        def _():
            for copy in hidden_loads(b + HIDDEN_SLOTS, slot):
                copy.start()
        return carry

    lax.fori_loop(0, HIDDEN_BLOCKS, hidden_step, 0)

    returns = [send(outgoing.at[c], incoming.at[c], 2 + c, mate) for c in range(OUT_BLOCKS)]
    if last:
        spreads = [send(x_new.at[c], x_far.at[c], 2 + OUT_BLOCKS + c, peer) for c in range(OUT_BLOCKS)]

    def finish(c):
        returns[c].wait_recv()
        cols = slice(c * o_block, (c + 1) * o_block)
        fresh = (x_mid[:, cols].astype(F32) + (mine[:, cols] + incoming[c].astype(F32))).astype(BF16)
        if last:
            x_new[c] = fresh
            spreads[c].start()
            out_own[:, cols] = fresh
        else:
            x_out[:, cols] = fresh

    for c in range(OUT_BLOCKS):
        down_load(c).wait()
        y = dot(hidden[...], downs[c])
        outgoing[c] = y[half:].astype(BF16)
        returns[c].start()
        mine[:, c * o_block:(c + 1) * o_block] = y[:half]
        if c:
            finish(c - 1)
    finish(OUT_BLOCKS - 1)

    if last:
        for c in range(OUT_BLOCKS):
            spreads[c].wait_recv()
            out_far[:, c * o_block:(c + 1) * o_block] = x_far[c]
            spreads[c].wait_send()
    else:
        for copy in loads:
            copy.wait()
        nxt = layer + 1
        low_rank(x_out[...], table_ref[own, :], attn_g[nxt:nxt + 1], kv_g[nxt:nxt + 1], q_g[nxt:nxt + 1], dkv, qa, low_mine)
        share = send(low_mine, low_far, 2 + OUT_BLOCKS, peer)
        share.start()
        low_out[own, :] = low_mine[...]
        share.wait_recv()
        low_out[far, :] = low_far[...]
        share.wait_send()
    scatter.wait_send()
    swap.wait_send()
    for c in range(OUT_BLOCKS):
        returns[c].wait_send()


def ffn(layer, last, part, x_in, table, ffn_gain, gains, w_gate, w_up, w_down, w_dkv_t, w_qa):
    rows, model = part.shape
    half = rows // 2
    h_width = w_gate.shape[2] // 2
    h_block = h_width // HIDDEN_BLOCKS
    o_block = model // OUT_BLOCKS
    padded = low_width(w_qa, w_dkv_t)
    scratch = [
        pltpu.VMEM((HIDDEN_SLOTS, model, 2 * h_block), BF16),
        pltpu.VMEM((OUT_BLOCKS, h_width, o_block), BF16),
        pltpu.VMEM((half, model), F32),
        pltpu.VMEM((half, model), BF16),
        pltpu.VMEM((rows, model), BF16),
        pltpu.VMEM((rows, h_width), BF16),
        pltpu.VMEM((half, model), F32),
        pltpu.VMEM((OUT_BLOCKS, half, o_block), BF16),
        pltpu.VMEM((OUT_BLOCKS, half, o_block), BF16),
    ]
    dma = pltpu.SemaphoreType.DMA
    if last:
        out_shape = (jax.ShapeDtypeStruct((half, model), BF16),) * 2
        out_specs = (VMEM, VMEM)
        scratch += [pltpu.VMEM((OUT_BLOCKS, half, o_block), BF16)] * 2 + [dma((2, HIDDEN_SLOTS)), dma((OUT_BLOCKS,))]
    else:
        out_shape = (jax.ShapeDtypeStruct((rows, padded), BF16), jax.ShapeDtypeStruct((half, model), BF16))
        out_specs = (VMEM, VMEM)
        scratch += [pltpu.VMEM((half, padded), BF16)] * 2 + [pltpu.VMEM(w_dkv_t.shape[1:], BF16), pltpu.VMEM(w_qa.shape[1:], BF16)]
        scratch += [dma((2, HIDDEN_SLOTS)), dma((OUT_BLOCKS,)), dma((2,))]
    copies = 2 + OUT_BLOCKS + (OUT_BLOCKS if last else 1)
    return pl.pallas_call(
        functools.partial(ffn_kernel, layer, last),
        out_shape=out_shape,
        in_specs=[VMEM] * 7 + [ANY] * 5,
        out_specs=out_specs,
        scratch_shapes=scratch + [dma((copies,)), dma((copies,))],
        compiler_params=pltpu.CompilerParams(vmem_limit_bytes=VMEM_LIMIT, collective_id=layer, has_side_effects=True),
        name="ffn",
    )(part, x_in, table, ffn_gain, *gains, w_gate, w_up, w_down, w_dkv_t, w_qa)


def solution(mesh):
    row_spec = P(('rep', 'dp'), None)
    cache_spec = P(('rep', 'dp'), None, None)
    in_specs = (row_spec, P(('rep', 'dp')), cache_spec, cache_spec, P(), P(), P(), P(), P(), P(), P(None, None, 'tp'), P(None, 'tp', None, None), P(None, 'tp', None, None), P(None, 'tp', None), P(), P(), P())
    out_specs = (row_spec, cache_spec, cache_spec)

    def local_step(x, lengths, cache0, cache1, attn_gain, kv_gain, q_gain, ffn_gain, w_dkv, w_qa, w_qb, w_uk, w_uv, w_o, w_gate, w_up, w_down):
        table = rope_tables(lengths, cache0.shape[2] - w_uk.shape[3])
        w_uv_t = jnp.swapaxes(w_uv, 2, 3)
        w_dkv_t = jnp.swapaxes(w_dkv, 1, 2)
        gains = (attn_gain, kv_gain, q_gain)
        caches = (cache0, cache1)
        given = x
        new_caches = []
        for i, cache in enumerate(caches):
            part, new_cache = attention(i, given, lengths, jnp.swapaxes(cache, 1, 2), table, gains, w_dkv_t, w_qa, w_qb, w_uk, w_uv_t, w_o)
            new_caches.append(jnp.swapaxes(new_cache, 1, 2))
            last = i == len(caches) - 1
            result = ffn(i, last, part, x, table, ffn_gain, gains, w_gate, w_up, w_down, w_dkv_t, w_qa)
            if not last:
                given, x = result
        mine, other = result
        x_out = jnp.where(lax.axis_index('tp') == 0, jnp.concatenate([mine, other], 0), jnp.concatenate([other, mine], 0))
        return x_out, new_caches[0], new_caches[1]

    return jax.shard_map(local_step, mesh=mesh, in_specs=in_specs, out_specs=out_specs, check_vma=False)
```

```python
import functools

import jax
import jax.numpy as jnp
from jax import lax
from jax.experimental import pallas as pl
from jax.experimental.pallas import tpu as pltpu
from jax.sharding import PartitionSpec as P

NORM_EPS = 1e-6
ROPE_BASE = 10000.0
F32 = jnp.float32
BF16 = jnp.bfloat16
ROWS_PER_STEP = 16
SLOTS = 5
OUT_SLOTS = 3
LANES = 128
PITCH_PAD = 8
HIDDEN_BLOCKS = 5
OUT_BLOCKS = 5
PIECES = 4
MESH = pl.DeviceIdType.MESH
VMEM_LIMIT = 60 * 1024 * 1024


def rms_norm(values, gain_vec):
    wide_vals = values.astype(F32)
    inv_rms = lax.rsqrt(jnp.mean(wide_vals * wide_vals, axis=-1, keepdims=True) + NORM_EPS)
    return (wide_vals * inv_rms * gain_vec).astype(BF16)


def rope_tables(lengths, rope_dim):
    half_dim = rope_dim // 2
    lane = jnp.arange(LANES)
    inv_freq = ROPE_BASE ** (-2.0 * (lane % half_dim).astype(F32) / rope_dim)
    angles = lengths.astype(F32)[:, None] * inv_freq[None, :]
    sines = jnp.sin(angles)
    return jnp.where(lane < rope_dim, jnp.cos(angles), jnp.where(lane % rope_dim < half_dim, -sines, sines))


def rotate(turn, table):
    half = turn.shape[1] // 2
    swapped = jnp.concatenate([turn[:, half:], turn[:, :half]], axis=1)
    return turn * table[:, :2 * half] + swapped * table[:, 2 * half:4 * half]


def dot(a, b):
    return jnp.dot(a, b, preferred_element_type=F32)


def dot_nt(a, b):
    return lax.dot_general(a, b, (((1,), (1,)), ((), ())), preferred_element_type=F32)


def low_query(normed, q_g, qa, out):
    out[...] = rms_norm(dot(normed, qa[...]), q_g)


def low_entry(normed, table, kv_g, dkv, out):
    latent = kv_g.shape[1]
    width = dkv.shape[0]
    kv_lat = dot_nt(normed, dkv[...])
    out[:, :latent] = rms_norm(kv_lat[:, :latent], kv_g)
    turned = rotate(kv_lat[:, latent:], table).astype(BF16)
    pad = jnp.zeros((normed.shape[0], out.shape[1] - width), BF16)
    out[:, latent:] = jnp.concatenate([turned, pad], axis=1)


def attention_kernel(layer, heads, nope, latent, lengths, given, table_ref, attn_g, kv_g, q_g, cache, w_dkv, w_qa, w_qb, w_uk, w_uv, w_o, part, new_cache,
                     blocks, outs, low, dkv, qa, qb, uk, uv, wo, entry, q_lat, q_rot, o_lat, o_cat, wsem, rsem, ssem):
    rows = table_ref.shape[0]
    pitch = rows + PITCH_PAD
    slots = cache.shape[2]
    width = cache.shape[1]
    rope = width - latent
    qk = nope + rope
    q_rank = qb.shape[0]
    steps = rows // ROWS_PER_STEP
    weights = [(w_dkv, dkv), (w_qa, qa), (w_qb, qb), (w_uk, uk), (w_uv, uv), (w_o, wo)]

    def load_weight(n):
        return pltpu.make_async_copy(weights[n][0].at[layer], weights[n][1], wsem.at[n])

    def row_slice(step):
        return pl.ds(pl.multiple_of(step * ROWS_PER_STEP, ROWS_PER_STEP), ROWS_PER_STEP)

    def load(step, slot):
        return pltpu.make_async_copy(cache.at[row_slice(step)], blocks.at[slot], rsem.at[slot])

    def store(step, slot):
        return pltpu.make_async_copy(outs.at[slot], new_cache.at[row_slice(step)], ssem.at[slot])

    first = layer == 0
    for n in ((0, 1) if first else ()) + (2, 3):
        load_weight(n).start()
    for step in range(SLOTS):
        load(step, step).start()
    load_weight(4).start()
    load_weight(5).start()

    table = table_ref[...]
    if first:
        load_weight(0).wait()
        load_weight(1).wait()
        normed = rms_norm(given[...], attn_g[layer:layer + 1])
        low_query(normed, q_g[layer:layer + 1], qa, low.at[:, :q_rank])
        low_entry(normed, table, kv_g[layer:layer + 1], dkv, low.at[:, q_rank:])
    else:
        low = given
    entry[...] = low[:, q_rank:].astype(F32)
    load_weight(2).wait()
    load_weight(3).wait()
    group = 4
    for g in range(heads // group):
        q_part = dot(low[:, :q_rank], qb[:, g * group * qk:(g + 1) * group * qk])
        for j in range(group):
            h = g * group + j
            mine = q_part[:, j * qk:(j + 1) * qk]
            q_rot[h * pitch:h * pitch + rows, :] = jnp.concatenate([rotate(mine[:, nope:], table).astype(BF16).astype(F32), jnp.zeros((rows, LANES - rope), F32)], axis=1)
            latent_q = dot(mine[:, :nope].astype(BF16), uk[h])
            for c in range(latent // LANES):
                q_lat[c, h * pitch:h * pitch + rows, :] = latent_q[:, c * LANES:(c + 1) * LANES].astype(BF16).astype(F32)

    scale = qk ** -0.5
    lane = lax.broadcasted_iota(jnp.int32, (1, slots), 1)

    def one_step(step, carry):
        slot = lax.rem(step, SLOTS)
        load(step, slot).wait()
        drain = lax.rem(step, OUT_SLOTS)

        @pl.when(step >= OUT_SLOTS)
        def _():
            store(step - OUT_SLOTS, drain).wait()

        fresh_rows = entry[row_slice(step), :]
        columns = jnp.transpose(fresh_rows)
        scores, probs, news = [], [], []
        for r in range(ROWS_PER_STEP):
            row = step * ROWS_PER_STEP + r
            lat = jnp.concatenate([q_lat.at[c][pl.ds(row, heads, stride=pitch), :] for c in range(latent // LANES)], axis=1)
            rot = q_rot[pl.ds(row, heads, stride=pitch), :]
            new_score = lat * fresh_rows[r:r + 1, :latent]
            new_score = jnp.sum(new_score[:, :LANES] + new_score[:, LANES:] + rot * fresh_rows[r:r + 1, latent:], axis=1, keepdims=True)
            score = dot(lat.astype(BF16), blocks[slot, r, :latent]) + dot(rot[:, :rope].astype(BF16), blocks[slot, r, latent:])
            scores.append(score)
            news.append(new_score)
        for r in range(ROWS_PER_STEP):
            length = lengths[step * ROWS_PER_STEP + r]
            new_score = news[r] * scale
            score = jnp.where(lane < length, scores[r] * scale, -1e30)
            top = jnp.maximum(jnp.max(score, axis=1, keepdims=True), new_score)
            score = jnp.exp(score - top)
            new_score = jnp.exp(new_score - top)
            inverse = 1.0 / (jnp.sum(score, axis=1, keepdims=True) + new_score)
            probs.append((score * inverse).astype(BF16))
            news[r] = (new_score * inverse).astype(BF16).astype(F32)
        for r in range(ROWS_PER_STEP):
            row = step * ROWS_PER_STEP + r
            mixed = dot_nt(probs[r], blocks[slot, r, :latent]) + news[r] * fresh_rows[r:r + 1, :latent]
            for c in range(latent // LANES):
                o_lat.at[c][pl.ds(row, heads, stride=pitch), :] = mixed[:, c * LANES:(c + 1) * LANES]
        for r in range(ROWS_PER_STEP):
            length = lengths[step * ROWS_PER_STEP + r]
            fresh = jnp.broadcast_to(columns[:width, r:r + 1], (width, slots)).astype(BF16)
            outs[drain, r] = jnp.where(lane == length, fresh, blocks[slot, r])
        store(step, drain).start()

        @pl.when(step + SLOTS < steps)
        def _():
            load(step + SLOTS, slot).start()
        return carry

    lax.fori_loop(0, steps, one_step, 0)
    load_weight(4).wait()
    load_weight(5).wait()
    for h in range(0, heads, 2):
        pair = []
        for n in (h, h + 1):
            mixed = jnp.concatenate([o_lat[c, n * pitch:n * pitch + rows, :] for c in range(latent // LANES)], axis=1)
            pair.append(dot_nt(mixed.astype(BF16), uv[n]).astype(BF16))
        v = uv.shape[1]
        o_cat[:, h * v:(h + 2) * v] = jnp.concatenate(pair, axis=1)
    chunk = 512
    for n in range(wo.shape[1] // chunk):
        part[:, n * chunk:(n + 1) * chunk] = dot(o_cat[...], wo[:, n * chunk:(n + 1) * chunk])
    for step in range(max(steps - OUT_SLOTS, 0), steps):
        store(step, step % OUT_SLOTS).wait()


ANY = pl.BlockSpec(memory_space=pl.ANY)
VMEM = pl.BlockSpec(memory_space=pltpu.VMEM)
SMEM = pl.BlockSpec(memory_space=pltpu.SMEM)


def low_width(w_qa, w_dkv_t):
    return -(-(w_qa.shape[2] + w_dkv_t.shape[1]) // LANES) * LANES


def attention(layer, given, lengths, cache_t, table, gains, w_dkv_t, w_qa, w_qb, w_uk, w_uv_t, w_o):
    rows = lengths.shape[0]
    _, heads, nope, latent = w_uk.shape
    width, slots = cache_t.shape[1:]
    model = w_o.shape[2]
    padded = low_width(w_qa, w_dkv_t)
    q_rank = w_qa.shape[2]
    low_shapes = [((rows, padded), BF16), (w_dkv_t.shape[1:], BF16), (w_qa.shape[1:], BF16)]
    if layer:
        low_shapes = [((8, LANES), BF16)] * 3
    return pl.pallas_call(
        functools.partial(attention_kernel, layer, heads, nope, latent),
        out_shape=(jax.ShapeDtypeStruct((rows, model), F32), jax.ShapeDtypeStruct(cache_t.shape, BF16)),
        in_specs=[SMEM] + [VMEM] * 5 + [ANY] * 7,
        out_specs=(VMEM, ANY),
        scratch_shapes=[pltpu.VMEM((n, ROWS_PER_STEP, width, slots), BF16) for n in (SLOTS, OUT_SLOTS)] + [pltpu.VMEM(*s) for s in low_shapes] + [
            pltpu.VMEM(w_qb.shape[1:], BF16),
            pltpu.VMEM(w_uk.shape[1:], BF16),
            pltpu.VMEM(w_uv_t.shape[1:], BF16),
            pltpu.VMEM(w_o.shape[1:], BF16),
            pltpu.VMEM((rows, padded - q_rank), F32),
            pltpu.VMEM((latent // LANES, heads * (rows + PITCH_PAD), LANES), F32),
            pltpu.VMEM((heads * (rows + PITCH_PAD), LANES), F32),
            pltpu.VMEM((latent // LANES, heads * (rows + PITCH_PAD), LANES), F32),
            pltpu.VMEM((rows, w_o.shape[1]), BF16),
            pltpu.SemaphoreType.DMA((6,)),
            pltpu.SemaphoreType.DMA((SLOTS,)),
            pltpu.SemaphoreType.DMA((OUT_SLOTS,)),
        ],
        compiler_params=pltpu.CompilerParams(vmem_limit_bytes=VMEM_LIMIT),
        name="attention",
    )(lengths, given, table, *gains, cache_t, w_dkv_t, w_qa, w_qb, w_uk, w_uv_t, w_o)


def ffn_kernel(layer, last, part, x_in, table_ref, ffn_g, attn_g, kv_g, q_g, w_gate, w_up, w_down, w_dkv, w_qa, *rest):
    if last:
        out_own, out_far, *rest = rest
        wides, downs, kept, ksem, arrived, x_mid, g_pair, hidden, mine, outgoing, incoming, x_new, x_far, sems, dsem, ssem, rsem = rest
    else:
        low_out, x_out, *rest = rest
        wides, downs, kept, ksem, arrived, x_mid, g_pair, hidden, mine, outgoing, incoming, q_mine, q_far, kv_mine, kv_far, dkv, qa, sems, dsem, lsem, ssem, rsem = rest
    tp = lax.axis_index("tp")
    dp = lax.axis_index("dp")
    core = lax.rem(dp, 2)
    peer = {"tp": 1 - tp}
    mate = {"dp": dp + 1 - 2 * core}
    half, model = arrived.shape
    h_slots = wides.shape[0]
    h_block = wides.shape[2] // 2
    h_width = hidden.shape[1]
    o_block = downs.shape[2]
    own = pl.ds(pl.multiple_of(tp * half, half), half)
    far = pl.ds(pl.multiple_of((1 - tp) * half, half), half)

    def hidden_loads(b, slot):
        cols = pl.ds(pl.multiple_of(core * h_width + b * h_block, LANES), h_block)
        return [pltpu.make_async_copy(w.at[layer, :, cols], wides.at[slot, :, pl.ds(n * h_block, h_block)], sems.at[n, slot]) for n, w in enumerate((w_gate, w_up))]

    def down_load(c):
        return pltpu.make_async_copy(w_down.at[layer, pl.ds(pl.multiple_of(core * h_width, LANES), h_width), pl.ds(c * o_block, o_block)], downs.at[c], dsem.at[c])

    barrier = pltpu.get_barrier_semaphore()
    for other in (peer, mate):
        pl.semaphore_signal(barrier, inc=1, device_id=other, device_id_type=MESH)
    for b in range(h_slots):
        for copy in hidden_loads(b, b):
            copy.start()
    for c in range(OUT_BLOCKS):
        down_load(c).start()
    if not last:
        loads = [pltpu.make_async_copy(w_dkv.at[layer + 1], dkv, lsem.at[0]), pltpu.make_async_copy(w_qa.at[layer + 1], qa, lsem.at[1])]
        for copy in loads:
            copy.start()

    pl.semaphore_wait(barrier, 2)

    def send(src, dst, n, to):
        return pltpu.make_async_remote_copy(src_ref=src, dst_ref=dst, send_sem=ssem.at[n], recv_sem=rsem.at[n], device_id=to, device_id_type=MESH)

    keep = pltpu.make_async_copy(part.at[own], kept, ksem)
    keep.start()
    piece = half // PIECES
    scatters, swaps = [], []
    for n in range(PIECES):
        rows = slice(n * piece, (n + 1) * piece)
        start = pl.multiple_of((1 - tp) * half + n * piece, piece)
        scatters.append(send(part.at[pl.ds(start, piece)], arrived.at[rows], n, peer))
        swaps.append(send(g_pair.at[rows], g_pair.at[half + n * piece:half + (n + 1) * piece], PIECES + n, mate))
        scatters[n].start()
    keep.wait()
    for n in range(PIECES):
        rows = slice(n * piece, (n + 1) * piece)
        mine_rows = pl.ds(pl.multiple_of(tp * half + n * piece, piece), piece)
        x_own = x_in[mine_rows, :] if layer == 0 else x_in[rows, :]
        scatters[n].wait_recv()
        mid = (x_own.astype(F32) + (kept[rows, :] + arrived[rows, :])).astype(BF16)
        x_mid[rows, :] = mid
        g_pair[rows, :] = rms_norm(mid, ffn_g[layer:layer + 1])
        swaps[n].start()
    for n in range(PIECES):
        swaps[n].wait_recv()

    def hidden_step(b, carry):
        slot = lax.rem(b, h_slots)
        for copy in hidden_loads(b, slot):
            copy.wait()
        both = dot(g_pair[...], wides[slot])
        gate, up = both[:, :h_block], both[:, h_block:]
        hidden[:, pl.ds(pl.multiple_of(b * h_block, LANES), h_block)] = (jax.nn.silu(gate) * up).astype(BF16)

        @pl.when(b + h_slots < HIDDEN_BLOCKS)
        def _():
            for copy in hidden_loads(b + h_slots, slot):
                copy.start()
        return carry

    lax.fori_loop(0, HIDDEN_BLOCKS, hidden_step, 0)

    returns = [send(outgoing.at[c], incoming.at[c], 2 * PIECES + c, mate) for c in range(OUT_BLOCKS)]
    if last:
        spreads = [send(x_new.at[c], x_far.at[c], 2 * PIECES + OUT_BLOCKS + c, peer) for c in range(OUT_BLOCKS)]

    def finish(c):
        returns[c].wait_recv()
        cols = slice(c * o_block, (c + 1) * o_block)
        fresh = (x_mid[:, cols].astype(F32) + (mine[:, cols] + incoming[c].astype(F32))).astype(BF16)
        if last:
            x_new[c] = fresh
            spreads[c].start()
            out_own[:, cols] = fresh
        else:
            x_out[:, cols] = fresh

    for c in range(OUT_BLOCKS):
        down_load(c).wait()
        y = dot(hidden[...], downs[c])
        outgoing[c] = y[half:].astype(BF16)
        returns[c].start()
        mine[:, c * o_block:(c + 1) * o_block] = y[:half]
        if c:
            finish(c - 1)
    finish(OUT_BLOCKS - 1)

    if last:
        for c in range(OUT_BLOCKS):
            spreads[c].wait_recv()
            out_far[:, c * o_block:(c + 1) * o_block] = x_far[c]
            spreads[c].wait_send()
    else:
        for copy in loads:
            copy.wait()
        nxt = layer + 1
        q_rank = qa.shape[1]
        shares = [send(a, b, 2 * PIECES + OUT_BLOCKS + n, peer) for n, (a, b) in enumerate(((q_mine, q_far), (kv_mine, kv_far)))]
        normed = rms_norm(x_out[...], attn_g[nxt:nxt + 1])
        low_query(normed, q_g[nxt:nxt + 1], qa, q_mine)
        shares[0].start()
        low_entry(normed, table_ref[own, :], kv_g[nxt:nxt + 1], dkv, kv_mine)
        shares[1].start()
        low_out[own, :q_rank] = q_mine[...]
        low_out[own, q_rank:] = kv_mine[...]
        shares[0].wait_recv()
        low_out[far, :q_rank] = q_far[...]
        shares[1].wait_recv()
        low_out[far, q_rank:] = kv_far[...]
        for share in shares:
            share.wait_send()
    for n in range(PIECES):
        scatters[n].wait_send()
        swaps[n].wait_send()
    for c in range(OUT_BLOCKS):
        returns[c].wait_send()


def ffn(layer, last, part, x_in, table, ffn_gain, gains, w_gate, w_up, w_down, w_dkv_t, w_qa):
    rows, model = part.shape
    half = rows // 2
    h_width = w_gate.shape[2] // 2
    h_block = h_width // HIDDEN_BLOCKS
    h_slots = HIDDEN_BLOCKS if last else HIDDEN_BLOCKS - 1
    o_block = model // OUT_BLOCKS
    padded = low_width(w_qa, w_dkv_t)
    scratch = [
        pltpu.VMEM((h_slots, model, 2 * h_block), BF16),
        pltpu.VMEM((OUT_BLOCKS, h_width, o_block), BF16),
        pltpu.VMEM((half, model), F32),
        pltpu.SemaphoreType.DMA(()),
        pltpu.VMEM((half, model), F32),
        pltpu.VMEM((half, model), BF16),
        pltpu.VMEM((rows, model), BF16),
        pltpu.VMEM((rows, h_width), BF16),
        pltpu.VMEM((half, model), F32),
        pltpu.VMEM((OUT_BLOCKS, half, o_block), BF16),
        pltpu.VMEM((OUT_BLOCKS, half, o_block), BF16),
    ]
    dma = pltpu.SemaphoreType.DMA
    if last:
        out_shape = (jax.ShapeDtypeStruct((half, model), BF16),) * 2
        out_specs = (VMEM, VMEM)
        scratch += [pltpu.VMEM((OUT_BLOCKS, half, o_block), BF16)] * 2 + [dma((2, h_slots)), dma((OUT_BLOCKS,))]
    else:
        out_shape = (jax.ShapeDtypeStruct((rows, padded), BF16), jax.ShapeDtypeStruct((half, model), BF16))
        out_specs = (VMEM, VMEM)
        q_rank = w_qa.shape[2]
        scratch += [pltpu.VMEM((half, q_rank), BF16)] * 2 + [pltpu.VMEM((half, padded - q_rank), BF16)] * 2 + [pltpu.VMEM(w_dkv_t.shape[1:], BF16), pltpu.VMEM(w_qa.shape[1:], BF16)]
        scratch += [dma((2, h_slots)), dma((OUT_BLOCKS,)), dma((2,))]
    copies = 2 * PIECES + OUT_BLOCKS + (OUT_BLOCKS if last else 2)
    return pl.pallas_call(
        functools.partial(ffn_kernel, layer, last),
        out_shape=out_shape,
        in_specs=[ANY] + [VMEM] * 6 + [ANY] * 5,
        out_specs=out_specs,
        scratch_shapes=scratch + [dma((copies,)), dma((copies,))],
        compiler_params=pltpu.CompilerParams(vmem_limit_bytes=VMEM_LIMIT, collective_id=layer, has_side_effects=True),
        name="ffn",
    )(part, x_in, table, ffn_gain, *gains, w_gate, w_up, w_down, w_dkv_t, w_qa)


def solution(mesh):
    row_spec = P(('rep', 'dp'), None)
    cache_spec = P(('rep', 'dp'), None, None)
    in_specs = (row_spec, P(('rep', 'dp')), cache_spec, cache_spec, P(), P(), P(), P(), P(), P(), P(None, None, 'tp'), P(None, 'tp', None, None), P(None, 'tp', None, None), P(None, 'tp', None), P(), P(), P())
    out_specs = (row_spec, cache_spec, cache_spec)

    def local_step(x, lengths, cache0, cache1, attn_gain, kv_gain, q_gain, ffn_gain, w_dkv, w_qa, w_qb, w_uk, w_uv, w_o, w_gate, w_up, w_down):
        table = rope_tables(lengths, cache0.shape[2] - w_uk.shape[3])
        w_uv_t = jnp.swapaxes(w_uv, 2, 3)
        w_dkv_t = jnp.swapaxes(w_dkv, 1, 2)
        gains = (attn_gain, kv_gain, q_gain)
        caches = (cache0, cache1)
        given = x
        new_caches = []
        for i, cache in enumerate(caches):
            part, new_cache = attention(i, given, lengths, jnp.swapaxes(cache, 1, 2), table, gains, w_dkv_t, w_qa, w_qb, w_uk, w_uv_t, w_o)
            new_caches.append(jnp.swapaxes(new_cache, 1, 2))
            last = i == len(caches) - 1
            result = ffn(i, last, part, x, table, ffn_gain, gains, w_gate, w_up, w_down, w_dkv_t, w_qa)
            if not last:
                given, x = result
        mine, other = result
        x_out = jnp.where(lax.axis_index('tp') == 0, jnp.concatenate([mine, other], 0), jnp.concatenate([other, mine], 0))
        return x_out, new_caches[0], new_caches[1]

    return jax.shard_map(local_step, mesh=mesh, in_specs=in_specs, out_specs=out_specs, check_vma=False)
```
